256 devices in a mesh: groups: 2 (over y), blk: 128 (over z, x, core).
Axes of the slice: x: 4, y: 2, z: 16, core: 2. Of those that a mesh axis runs over, the one named last changes fastest.
The devices are a block of a 4x16x16 slice.
Arguments:
- queries: bfloat16 [65536, 2560], P(('groups', 'blk')), parts along dimension 0
- keys: bfloat16 [65536, 2560], P(('groups', 'blk')), parts along dimension 0
- values: bfloat16 [65536, 2560], P(('groups', 'blk')), parts along dimension 0
- out_weight: bfloat16 [64, 2560], replicated, may hold values from -0.125 to 0.125
- latent: float32 [64, 65536], P(None, ('groups', 'blk')), parts along dimension 1, may hold values from -6 to 6
- valid: int32 [256], P('groups'), parts along dimension 0, may hold values from 64 to 256, as said below
- timestep: int32 [2], P('groups'), parts along dimension 0, may hold values from 0 to 9
Outputs:
- velocity: float32 [64, 65536], P(None, ('groups', 'blk')), parts along dimension 1
- latent_next: float32 [64, 65536], P(None, ('groups', 'blk')), parts along dimension 1
The draws below stay inside these ranges and needn't reach their ends.
There are 2 independent parts, one for each index of `groups`. The reference program is written for one: setup_inputs(seed, part) draws one part's arguments, and reference() takes and returns one part's arrays. A program takes and returns all parts, laid end to end along the dimension named above; an argument that names none is the same for every part. Nothing has to cross between parts.
Inputs may be any that keep to these rules, and one draw needn't show every extreme that they name: `valid`: blocks whose index is one less than a multiple of 4 hold between 64 and 256 used tokens; all other blocks are full.
All inputs are finite; a program needn't handle non-finite values.
Results may differ from the reference program's by a relative error of at most 0.0065.
Values may be sent and summed in bfloat16 or wider, within the bound.
No kernel may reach another device: no remote copies, remote signals or barrier semaphores. Data moves between devices by JAX's collectives and lax.ppermute only.
A program may use at most 128 MiB of HBM per device.

```python
import jax
import jax.numpy as jnp
from jax import lax

HEADS = 20
HEAD_DIM = 128
LATENT_CH = 64
TOK_DEV = 256
R_WIN = 2
FRAME_BLOCKS = 4
STEPS = 10
BLOCKS = 128
TOKENS = 32768
FEATURES = 2560


def draw_queries(key, part):
    base = jax.random.normal(jax.random.fold_in(key, 3), (TOKENS, HEADS * HEAD_DIM), jnp.float32)
    return base.astype(jnp.bfloat16)


def draw_keys(key, part):
    base = jax.random.normal(jax.random.fold_in(key, 5), (TOKENS, HEADS * HEAD_DIM), jnp.float32)
    return base.astype(jnp.bfloat16)


def draw_values(key, part):
    position = jnp.arange(TOKENS, dtype=jnp.float32)[:, None] / TOKENS
    entries = jax.random.normal(jax.random.fold_in(key, 7), (TOKENS, HEADS * HEAD_DIM), jnp.float32)
    base = entries * (0.6 + 1.4 * position)
    return jnp.clip(base, -8.0, 8.0).astype(jnp.bfloat16)


def draw_valid(key, part):
    counts = jax.random.randint(jax.random.fold_in(key, 11), (BLOCKS,), TOK_DEV // 4, TOK_DEV + 1, jnp.int32)
    ending = jnp.arange(BLOCKS, dtype=jnp.int32) % FRAME_BLOCKS == FRAME_BLOCKS - 1
    return jnp.where(ending, counts, jnp.int32(TOK_DEV))


def levels(own_key, dims, pieces, smallest, largest):
    def one(axis_at, parts):
        steps = jax.random.uniform(jax.random.fold_in(jax.random.fold_in(own_key, 6), axis_at), (parts,), jnp.float32, smallest / len(pieces), largest / len(pieces))
        return jnp.repeat(jnp.exp(steps), dims[axis_at] // parts).reshape((-1,) + (1,) * (len(dims) - axis_at - 1))

    factor_of = one(*pieces[0])
    for cut in pieces[1:]:
        factor_of = factor_of * one(*cut)
    return factor_of


def gaussian(own_key, dims, deviation, most, split=(), held_as=jnp.bfloat16):
    values = deviation * jax.random.normal(own_key, dims, jnp.float32)
    if split:
        values = values * levels(own_key, dims, split, -0.22, 0.18)
    return jnp.clip(values, -most, most).astype(held_as)


def setup_inputs(seed: int = 0, part: int = 0) -> dict:
    key_list = jax.random.split(jax.random.key(seed), 8)
    own_keys = jax.random.split(jax.random.fold_in(key_list[7], part), 8)
    return {
        "queries": draw_queries(jax.random.fold_in(jax.random.fold_in(key_list[7], part), 71), part),
        "keys": draw_keys(jax.random.fold_in(jax.random.fold_in(key_list[7], part), 71), part),
        "values": draw_values(jax.random.fold_in(jax.random.fold_in(key_list[7], part), 71), part),
        "out_weight": gaussian(key_list[3], (LATENT_CH, FEATURES), FEATURES ** -0.5, 0.125),
        "latent": gaussian(own_keys[4], (LATENT_CH, TOKENS), 1.0, 6.0, ((1, 128),), jnp.float32),
        "valid": draw_valid(jax.random.fold_in(jax.random.fold_in(key_list[7], part), 71), part),
        "timestep": jax.random.randint(own_keys[6], (1,), 0, STEPS).astype(jnp.int32),
    }


def reference(queries, keys, values, out_weight, latent, valid, timestep):
    span = (2 * R_WIN + 1) * TOK_DEV
    zero_rows = jnp.zeros((R_WIN * TOK_DEV, HEADS * HEAD_DIM), jnp.bfloat16)
    keys_padded = jnp.concatenate([zero_rows, keys, zero_rows], axis=0)
    values_padded = jnp.concatenate([zero_rows, values, zero_rows], axis=0)
    zero_counts = jnp.zeros((R_WIN,), jnp.int32)
    valid_padded = jnp.concatenate([zero_counts, valid.astype(jnp.int32), zero_counts], axis=0)
    slots = jnp.arange(TOK_DEV, dtype=jnp.int32)
    score_scale = 1.0 / jnp.sqrt(jnp.float32(HEAD_DIM))

    def one_block(block):
        start = (block * TOK_DEV).astype(jnp.int32)
        query_heads = lax.dynamic_slice_in_dim(queries, start, TOK_DEV, 0).reshape(TOK_DEV, HEADS, HEAD_DIM).astype(jnp.float32)
        key_heads = lax.dynamic_slice_in_dim(keys_padded, start, span, 0).reshape(span, HEADS, HEAD_DIM).astype(jnp.float32)
        value_heads = lax.dynamic_slice_in_dim(values_padded, start, span, 0).reshape(span, HEADS, HEAD_DIM).astype(jnp.float32)
        counts = lax.dynamic_slice_in_dim(valid_padded, block.astype(jnp.int32), 2 * R_WIN + 1, 0)
        key_used = (slots[None, :] < counts[:, None]).reshape(span)
        scores = jnp.einsum('qhd,khd->hqk', query_heads, key_heads) * score_scale
        scores = jnp.where(key_used[None, None, :], scores, jnp.float32(-1e+30))
        top = lax.optimization_barrier(jnp.max(scores, axis=-1, keepdims=True))
        weights = jnp.exp(scores - top)
        total = lax.optimization_barrier(jnp.sum(weights, axis=-1))
        rounded = weights.astype(jnp.bfloat16).astype(jnp.float32)
        mixed = jnp.einsum('hqk,khd->hqd', rounded, value_heads) / total[:, :, None]
        mixed = jnp.transpose(mixed, (1, 0, 2)).reshape(TOK_DEV, HEADS * HEAD_DIM)
        used = slots < valid[block]
        attn = jnp.where(used[:, None], mixed, 0.0).astype(jnp.bfloat16)
        return lax.dot_general(out_weight, attn, (((1,), (1,)), ((), ())), preferred_element_type=jnp.float32)
    blocks_vel = lax.map(one_block, jnp.arange(BLOCKS, dtype=jnp.int32))
    vel = jnp.transpose(blocks_vel, (1, 0, 2)).reshape(LATENT_CH, TOKENS)
    squares = jnp.sum(vel * vel)
    count = jnp.float32(LATENT_CH) * jnp.sum(valid.astype(jnp.float32))
    rms = jnp.sqrt(squares / count + 1e-06)
    velocity = vel / rms
    level = timestep[0].astype(jnp.float32)
    early = 1.0 - level / STEPS
    later = 1.0 - (level + 1.0) / STEPS
    sigma_early = 5.0 * early / (1.0 + 4.0 * early)
    sigma_later = 5.0 * later / (1.0 + 4.0 * later)
    latent_next = latent + (sigma_later - sigma_early) * velocity
    return (velocity, latent_next)
```

```python
import functools
import math

import jax
import jax.numpy as jnp
from jax import lax
from jax.experimental import pallas as pl
from jax.experimental.pallas import tpu as pltpu
from jax.sharding import Mesh
from jax.sharding import PartitionSpec as P

HEADS = 20
HEAD_DIM = 128
LATENT_CH = 64
PAIRS = HEADS // 2
LANES = 2 * LATENT_CH
STEPS = 10
Z_CORE = ("blk_0", "blk_2")
BLK = ("blk_0", "blk_1", "blk_2")
GROUPS_BLK = ("groups", "blk_0", "blk_1", "blk_2")
SCORE_SCALE = math.log2(math.e) / math.sqrt(HEAD_DIM)
LARGEST = 3.3e38


def dot_last(left, right):
    return lax.dot_general(
        left, right, (((1,), (1,)), ((), ())), preferred_element_type=jnp.float32
    )


def dot_plain(left, right):
    return jnp.dot(left, right, preferred_element_type=jnp.float32)


def project_kernel(counts, values, weight, out):
    rows = values.shape[0]
    used = lax.broadcasted_iota(jnp.int32, values.shape, 0) < counts[0]
    kept = jnp.where(used, values[...], jnp.zeros_like(values))
    pair = weight[...]
    even = lax.broadcasted_iota(jnp.int32, pair.shape, 1) < HEAD_DIM
    zero = jnp.zeros_like(pair)
    stacked = jnp.concatenate([jnp.where(even, pair, zero), jnp.where(even, zero, pair)], axis=0)
    projected = dot_last(kept, stacked)
    out[...] = jnp.clip(projected, -LARGEST, LARGEST).astype(jnp.bfloat16)


def project(counts, values, weight):
    rows = values.shape[0]
    return pl.pallas_call(
        project_kernel,
        grid=(PAIRS,),
        in_specs=[
            pl.BlockSpec(memory_space=pltpu.SMEM),
            pl.BlockSpec((rows, 2 * HEAD_DIM), lambda g: (0, g)),
            pl.BlockSpec((LATENT_CH, 2 * HEAD_DIM), lambda g: (0, g)),
        ],
        out_specs=pl.BlockSpec((rows, LANES), lambda g: (0, g)),
        out_shape=jax.ShapeDtypeStruct((rows, PAIRS * LANES), jnp.bfloat16),
        name="project",
    )(counts, values, weight)


def weights_kernel(counts, queries, *refs):
    keys, own_values = refs[:5], refs[5:7]
    remote, own_sum = refs[7:10], refs[10]
    even_sum, odd_sum = refs[11:13]
    step = pl.program_id(0)
    rows = queries.shape[0]
    columns = lax.broadcasted_iota(jnp.int32, (rows, rows), 1)

    @pl.when(step == 0)
    def _():
        even_sum[...] = jnp.zeros_like(even_sum)
        odd_sum[...] = jnp.zeros_like(odd_sum)

    for side in range(2):
        part = slice(side * HEAD_DIM, (side + 1) * HEAD_DIM)
        query = queries[:, part]
        scores = []
        for block in range(5):
            score = dot_last(query, keys[block][:, part]) * SCORE_SCALE
            scores.append(jnp.where(columns < counts[block], score, jnp.float32(-1e30)))
        top = functools.reduce(jnp.maximum, scores)
        top = jnp.max(top, axis=-1, keepdims=True)
        weights = [jnp.exp2(score - top) for score in scores]
        total = functools.reduce(jnp.add, weights)
        total = jnp.sum(total, axis=-1, keepdims=True)
        share = 1.0 / total
        shares = [(weight * share).astype(jnp.bfloat16) for weight in weights]
        for block in range(3):
            remote[block][side] = shares[2 + block]
        acc = (even_sum, odd_sum)[side]
        acc[...] += dot_plain(shares[0], own_values[0][...]) + dot_plain(
            shares[1], own_values[1][...]
        )

    @pl.when(step == PAIRS - 1)
    def _():
        low = lax.broadcasted_iota(jnp.int32, even_sum.shape, 1) < LATENT_CH
        own_sum[...] = jnp.where(low, even_sum[...], odd_sum[...])


def attention_weights(counts, queries, keys, own_values):
    rows = queries.shape[0]
    pair_columns = pl.BlockSpec((rows, 2 * HEAD_DIM), lambda g: (0, g))
    lanes = pl.BlockSpec((rows, LANES), lambda g: (0, g))
    share = pl.BlockSpec((2, rows, rows), lambda g: (g, 0, 0))
    share_shape = jax.ShapeDtypeStruct((HEADS, rows, rows), jnp.bfloat16)
    return pl.pallas_call(
        weights_kernel,
        grid=(PAIRS,),
        in_specs=[pl.BlockSpec(memory_space=pltpu.SMEM), pair_columns]
        + [pair_columns] * 5
        + [lanes] * 2,
        out_specs=[share] * 3 + [pl.BlockSpec((rows, LANES), lambda g: (0, 0))],
        out_shape=[share_shape] * 3 + [jax.ShapeDtypeStruct((rows, LANES), jnp.float32)],
        scratch_shapes=[pltpu.VMEM((rows, LANES), jnp.float32)] * 2,
        name="attention_weights",
    )(counts, queries, *keys, *own_values)


def gather_kernel(blocks, finish, *refs):
    shares, values = refs[:blocks], refs[blocks : 2 * blocks]
    start = refs[2 * blocks]
    rest = refs[2 * blocks + 1 :]
    if finish:
        counts, out, squares, even_sum, odd_sum = rest
    else:
        out, even_sum, odd_sum = rest
    step = pl.program_id(0)

    @pl.when(step == 0)
    def _():
        even_sum[...] = jnp.zeros_like(even_sum)
        odd_sum[...] = jnp.zeros_like(odd_sum)

    pairs = values[0].shape[1] // LANES
    for side in range(2):
        acc = (even_sum, odd_sum)[side]
        total = acc[...]
        for pair in range(pairs):
            for block in range(blocks):
                total += dot_plain(
                    shares[block][2 * pair + side],
                    values[block][:, pair * LANES : (pair + 1) * LANES],
                )
        acc[...] = total

    @pl.when(step == pl.num_programs(0) - 1)
    def _():
        low = lax.broadcasted_iota(jnp.int32, even_sum.shape, 1) < LATENT_CH
        both = start[...] + jnp.where(low, even_sum[...], odd_sum[...])
        if not finish:
            out[...] = both
        else:
            both = both + pltpu.roll(both, LATENT_CH, 1)
            vel = jnp.transpose(both)[:LATENT_CH]
            used = lax.broadcasted_iota(jnp.int32, vel.shape, 1) < counts[0]
            vel = jnp.where(used, vel, 0.0)
            out[...] = vel
            square = jnp.sum(vel * vel, axis=0, keepdims=True)
            squares[...] = jnp.broadcast_to(
                jnp.sum(square, axis=1, keepdims=True), squares.shape
            )


def gather(shares, values, start, counts=None):
    blocks = len(shares)
    finish = counts is not None
    rows = start.shape[0]
    pairs = 5
    steps = PAIRS // pairs
    whole = lambda g: (0, 0)
    in_specs = (
        [pl.BlockSpec((2 * pairs, rows, rows), lambda g: (g, 0, 0))] * blocks
        + [pl.BlockSpec((rows, pairs * LANES), lambda g: (0, g))] * blocks
        + [pl.BlockSpec((rows, LANES), whole)]
    )
    operands = [*shares, *values, start]
    if finish:
        in_specs.append(pl.BlockSpec(memory_space=pltpu.SMEM))
        operands.append(counts)
        out_specs = [pl.BlockSpec((LATENT_CH, rows), whole), pl.BlockSpec((1, LANES), whole)]
        out_shape = [
            jax.ShapeDtypeStruct((LATENT_CH, rows), jnp.float32),
            jax.ShapeDtypeStruct((1, LANES), jnp.float32),
        ]
    else:
        out_specs = pl.BlockSpec((rows, LANES), whole)
        out_shape = jax.ShapeDtypeStruct((rows, LANES), jnp.float32)
    return pl.pallas_call(
        functools.partial(gather_kernel, blocks, finish),
        grid=(steps,),
        in_specs=in_specs,
        out_specs=out_specs,
        out_shape=out_shape,
        scratch_shapes=[pltpu.VMEM((rows, LANES), jnp.float32)] * 2,
        name="gather_last" if finish else "gather_first",
    )(*operands)


def exchange(shard, pairs):
    return lax.ppermute(shard, BLK, pairs)


def total_over(row, axes):
    count = lax.axis_size(axes)
    copies = jnp.broadcast_to(row, (count, row.shape[1]))
    gathered = lax.all_to_all(copies, axes, 0, 0, tiled=True)
    return jnp.sum(gathered, axis=0, keepdims=True)


def local(queries, keys, values, out_weight, latent, valid, timestep):
    blocks = lax.axis_size(BLK)
    own = lax.axis_index(BLK)
    near_pairs = [((i + 2) % blocks if i % 2 == 0 else (i - 2) % blocks, i) for i in range(blocks)]
    far_pairs = [((i - 2) % blocks if i % 2 == 0 else (i + 2) % blocks, i) for i in range(blocks)]
    chip_pairs = [(i, i ^ 1) for i in range(blocks)]
    is_odd = own % 2
    partner = own + 1 - 2 * is_odd
    near = own + 2 - 4 * is_odd
    far = own - 2 + 4 * is_odd
    over = own - 1 + 2 * is_odd
    index = jnp.stack([own, partner, near, far, over])
    inside = (index >= 0) & (index < blocks)
    counts = jnp.where(inside, valid[jnp.clip(index, 0, blocks - 1)], 0).astype(jnp.int32)

    keys_near = exchange(keys, near_pairs)
    keys_far = exchange(keys, far_pairs)
    keys_partner = exchange(keys, chip_pairs)
    projected = project(counts, values, out_weight)
    projected_partner = exchange(projected, chip_pairs)
    projected_near = exchange(projected, near_pairs)
    projected_far = exchange(projected, far_pairs)
    keys_near, _ = lax.optimization_barrier((keys_near, projected))
    keys_over = exchange(keys_near, chip_pairs)
    shares_near, shares_far, shares_over, own_sum = attention_weights(
        counts,
        queries,
        (keys, keys_partner, keys_near, keys_far, keys_over),
        (projected, projected_partner),
    )
    projected_over = exchange(projected_near, chip_pairs)
    most = gather((shares_near, shares_far), (projected_near, projected_far), own_sum)
    vel, squares = gather((shares_over,), (projected_over,), most, counts)

    squares = total_over(total_over(squares, Z_CORE), "blk_1")[0, 0]
    count = jnp.float32(LATENT_CH) * jnp.sum(valid.astype(jnp.float32))
    rms = jnp.sqrt(squares / count + 1e-06)
    velocity = vel / rms
    level = timestep[0].astype(jnp.float32)
    early = 1.0 - level / STEPS
    later = 1.0 - (level + 1.0) / STEPS
    sigma_early = 5.0 * early / (1.0 + 4.0 * early)
    sigma_later = 5.0 * later / (1.0 + 4.0 * later)
    return (velocity, latent + (sigma_later - sigma_early) * velocity)


def solution(mesh):
    split = Mesh(
        mesh.devices.reshape(mesh.shape["groups"], 16, 4, 2), ("groups", "blk_0", "blk_1", "blk_2")
    )
    return jax.shard_map(
        local,
        mesh=split,
        in_specs=(
            P(GROUPS_BLK, None),
            P(GROUPS_BLK, None),
            P(GROUPS_BLK, None),
            P(),
            P(None, GROUPS_BLK),
            P("groups"),
            P("groups"),
        ),
        out_specs=(P(None, GROUPS_BLK), P(None, GROUPS_BLK)),
        check_vma=False,
    )
```

```python
import functools
import math

import jax
import jax.numpy as jnp
from jax import lax
from jax.experimental import pallas as pl
from jax.experimental.pallas import tpu as pltpu
from jax.sharding import Mesh
from jax.sharding import PartitionSpec as P


HEADS = 20
HEAD_DIM = 128
LATENT_CH = 64
PAIRS = HEADS // 2
LANES = 2 * LATENT_CH
STEPS = 10
Z_CORE = ("blk_0", "blk_2")
BLK = ("blk_0", "blk_1", "blk_2")
GROUPS_BLK = ("groups", "blk_0", "blk_1", "blk_2")
SCORE_SCALE = math.log2(math.e) / math.sqrt(HEAD_DIM)
LARGEST = 3.3e38


def dot_last(left, right):
    return lax.dot_general(
        left, right, (((1,), (1,)), ((), ())), preferred_element_type=jnp.float32
    )


def dot_plain(left, right):
    return jnp.dot(left, right, preferred_element_type=jnp.float32)


def project_kernel(counts, values, weight, out):
    used = lax.broadcasted_iota(jnp.int32, values.shape, 0) < counts[0]
    kept = jnp.where(used, values[...], jnp.zeros_like(values))
    pair = weight[...]
    even = lax.broadcasted_iota(jnp.int32, pair.shape, 1) < HEAD_DIM
    zero = jnp.zeros_like(pair)
    stacked = jnp.concatenate([jnp.where(even, pair, zero), jnp.where(even, zero, pair)], axis=0)
    projected = dot_last(kept, stacked)
    out[...] = jnp.clip(projected, -LARGEST, LARGEST).astype(jnp.bfloat16)


def project(counts, values, weight):
    rows = values.shape[0]
    return pl.pallas_call(
        project_kernel,
        grid=(PAIRS,),
        in_specs=[
            pl.BlockSpec(memory_space=pltpu.SMEM),
            pl.BlockSpec((rows, 2 * HEAD_DIM), lambda g: (0, g)),
            pl.BlockSpec((LATENT_CH, 2 * HEAD_DIM), lambda g: (0, g)),
        ],
        out_specs=pl.BlockSpec((rows, LANES), lambda g: (0, g)),
        out_shape=jax.ShapeDtypeStruct((rows, PAIRS * LANES), jnp.bfloat16),
        name="project",
    )(counts, values, weight)


def own_kernel(counts, queries, *refs):
    keys, projected = refs[:2], refs[2:4]
    sums, stats = refs[4:]
    rows = queries.shape[0]
    columns = lax.broadcasted_iota(jnp.int32, (rows, rows), 1)
    parts, tops, totals = [], [], []
    for side in range(2):
        part = slice(side * HEAD_DIM, (side + 1) * HEAD_DIM)
        query = queries[:, part]
        scores = []
        for block in range(2):
            score = dot_last(query, keys[block][:, part]) * SCORE_SCALE
            scores.append(jnp.where(columns < counts[block], score, jnp.float32(-1e30)))
        top = jnp.max(functools.reduce(jnp.maximum, scores), axis=-1, keepdims=True)
        weights = [jnp.exp2(score - top) for score in scores]
        tops.append(top)
        totals.append(jnp.sum(functools.reduce(jnp.add, weights), axis=-1, keepdims=True))
        parts.append(
            functools.reduce(
                jnp.add,
                [dot_plain(w.astype(jnp.bfloat16), v[...]) for w, v in zip(weights, projected)],
            )
        )
    low = lax.broadcasted_iota(jnp.int32, parts[0].shape, 1) < LATENT_CH
    sums[...] = jnp.where(low, parts[0], parts[1])
    lane = lax.broadcasted_iota(jnp.int32, stats.shape[1:], 1)
    stats[0] = jnp.where(
        lane < 2,
        jnp.where(lane == 0, tops[0], tops[1]),
        jnp.where(lane == 2, totals[0], totals[1]),
    )


def own_attention(counts, queries, keys, projected):
    rows = queries.shape[0]
    pair_columns = pl.BlockSpec((rows, 2 * HEAD_DIM), lambda g: (0, g))
    lanes = pl.BlockSpec((rows, LANES), lambda g: (0, g))
    return pl.pallas_call(
        own_kernel,
        grid=(PAIRS,),
        in_specs=[pl.BlockSpec(memory_space=pltpu.SMEM)] + [pair_columns] * 3 + [lanes] * 2,
        out_specs=[lanes, pl.BlockSpec((1, rows, 8), lambda g: (g, 0, 0))],
        out_shape=[
            jax.ShapeDtypeStruct((rows, PAIRS * LANES), jnp.float32),
            jax.ShapeDtypeStruct((PAIRS, rows, 8), jnp.float32),
        ],
        name="own_attention",
    )(counts, queries, *keys, *projected)


def weights_kernel(counts, queries, *refs):
    keys, sums, stats = refs[:3], refs[3], refs[4]
    remote, own_sum = refs[5:8], refs[8]
    step = pl.program_id(0)
    rows = queries.shape[0]
    columns = lax.broadcasted_iota(jnp.int32, (rows, rows), 1)

    @pl.when(step == 0)
    def _():
        own_sum[...] = jnp.zeros_like(own_sum)

    scales = []
    for side in range(2):
        part = slice(side * HEAD_DIM, (side + 1) * HEAD_DIM)
        query = queries[:, part]
        own_top = stats[0, :, side : side + 1]
        own_total = stats[0, :, 2 + side : 3 + side]
        scores = []
        for block in range(3):
            score = dot_last(query, keys[block][:, part]) * SCORE_SCALE
            scores.append(jnp.where(columns < counts[2 + block], score, jnp.float32(-1e30)))
        top = jnp.max(functools.reduce(jnp.maximum, scores), axis=-1, keepdims=True)
        top = jnp.maximum(top, own_top)
        shrink = jnp.exp2(own_top - top)
        weights = [jnp.exp2(score - top) for score in scores]
        total = jnp.sum(functools.reduce(jnp.add, weights), axis=-1, keepdims=True)
        share = 1.0 / (total + own_total * shrink)
        for block in range(3):
            remote[block][side] = (weights[block] * share).astype(jnp.bfloat16)
        scales.append(shrink * share)
    low = lax.broadcasted_iota(jnp.int32, own_sum.shape, 1) < LATENT_CH
    own_sum[...] += sums[...] * jnp.where(low, scales[0], scales[1])


def attention_weights(counts, queries, keys, sums, stats):
    rows = queries.shape[0]
    pair_columns = pl.BlockSpec((rows, 2 * HEAD_DIM), lambda g: (0, g))
    share = pl.BlockSpec((2, rows, rows), lambda g: (g, 0, 0))
    share_shape = jax.ShapeDtypeStruct((HEADS, rows, rows), jnp.bfloat16)
    return pl.pallas_call(
        weights_kernel,
        grid=(PAIRS,),
        in_specs=[pl.BlockSpec(memory_space=pltpu.SMEM)]
        + [pair_columns] * 4
        + [
            pl.BlockSpec((rows, LANES), lambda g: (0, g)),
            pl.BlockSpec((1, rows, 8), lambda g: (g, 0, 0)),
        ],
        out_specs=[share] * 3 + [pl.BlockSpec((rows, LANES), lambda g: (0, 0))],
        out_shape=[share_shape] * 3 + [jax.ShapeDtypeStruct((rows, LANES), jnp.float32)],
        name="attention_weights",
    )(counts, queries, *keys, sums, stats)


def gather_kernel(blocks, finish, *refs):
    shares, values = refs[:blocks], refs[blocks : 2 * blocks]
    start = refs[2 * blocks]
    rest = refs[2 * blocks + 1 :]
    if finish:
        counts, out, squares, even_sum, odd_sum = rest
    else:
        out, even_sum, odd_sum = rest
    step = pl.program_id(0)

    @pl.when(step == 0)
    def _():
        even_sum[...] = jnp.zeros_like(even_sum)
        odd_sum[...] = jnp.zeros_like(odd_sum)

    pairs = values[0].shape[1] // LANES
    for side in range(2):
        acc = (even_sum, odd_sum)[side]
        total = acc[...]
        for pair in range(pairs):
            for block in range(blocks):
                total += dot_plain(
                    shares[block][2 * pair + side],
                    values[block][:, pair * LANES : (pair + 1) * LANES],
                )
        acc[...] = total

    @pl.when(step == pl.num_programs(0) - 1)
    def _():
        low = lax.broadcasted_iota(jnp.int32, even_sum.shape, 1) < LATENT_CH
        both = start[...] + jnp.where(low, even_sum[...], odd_sum[...])
        if not finish:
            out[...] = both
        else:
            both = both + pltpu.roll(both, LATENT_CH, 1)
            vel = jnp.transpose(both)[:LATENT_CH]
            used = lax.broadcasted_iota(jnp.int32, vel.shape, 1) < counts[0]
            vel = jnp.where(used, vel, 0.0)
            out[...] = vel
            square = jnp.sum(vel * vel, axis=0, keepdims=True)
            squares[...] = jnp.broadcast_to(
                jnp.sum(square, axis=1, keepdims=True), squares.shape
            )


def gather(shares, values, start, counts=None):
    blocks = len(shares)
    finish = counts is not None
    rows = start.shape[0]
    pairs = 5
    steps = PAIRS // pairs
    whole = lambda g: (0, 0)
    in_specs = (
        [pl.BlockSpec((2 * pairs, rows, rows), lambda g: (g, 0, 0))] * blocks
        + [pl.BlockSpec((rows, pairs * LANES), lambda g: (0, g))] * blocks
        + [pl.BlockSpec((rows, LANES), whole)]
    )
    operands = [*shares, *values, start]
    if finish:
        in_specs.append(pl.BlockSpec(memory_space=pltpu.SMEM))
        operands.append(counts)
        out_specs = [pl.BlockSpec((LATENT_CH, rows), whole), pl.BlockSpec((1, LANES), whole)]
        out_shape = [
            jax.ShapeDtypeStruct((LATENT_CH, rows), jnp.float32),
            jax.ShapeDtypeStruct((1, LANES), jnp.float32),
        ]
    else:
        out_specs = pl.BlockSpec((rows, LANES), whole)
        out_shape = jax.ShapeDtypeStruct((rows, LANES), jnp.float32)
    return pl.pallas_call(
        functools.partial(gather_kernel, blocks, finish),
        grid=(steps,),
        in_specs=in_specs,
        out_specs=out_specs,
        out_shape=out_shape,
        scratch_shapes=[pltpu.VMEM((rows, LANES), jnp.float32)] * 2,
        name="gather_last" if finish else "gather_first",
    )(*operands)


def exchange(shard, pairs):
    return lax.ppermute(shard, BLK, pairs)


def total_over(row, axes):
    count = lax.axis_size(axes)
    copies = jnp.broadcast_to(row, (count, row.shape[1]))
    gathered = lax.all_to_all(copies, axes, 0, 0, tiled=True)
    return jnp.sum(gathered, axis=0, keepdims=True)


def step(queries, keys, values, out_weight, latent, valid, timestep):
    blocks = lax.axis_size(BLK)
    own = lax.axis_index(BLK)
    near_pairs = [((i + 2) % blocks if i % 2 == 0 else (i - 2) % blocks, i) for i in range(blocks)]
    far_pairs = [((i - 2) % blocks if i % 2 == 0 else (i + 2) % blocks, i) for i in range(blocks)]
    chip_pairs = [(i, i ^ 1) for i in range(blocks)]
    is_odd = own % 2
    partner = own + 1 - 2 * is_odd
    near = own + 2 - 4 * is_odd
    far = own - 2 + 4 * is_odd
    over = own - 1 + 2 * is_odd
    index = jnp.stack([own, partner, near, far, over])
    inside = (index >= 0) & (index < blocks)
    counts = jnp.where(inside, valid[jnp.clip(index, 0, blocks - 1)], 0).astype(jnp.int32)

    keys_near = exchange(keys, near_pairs)
    keys_far = exchange(keys, far_pairs)
    keys_partner = exchange(keys, chip_pairs)
    projected = project(counts, values, out_weight)
    projected_partner = exchange(projected, chip_pairs)
    sums, stats = own_attention(
        counts, queries, (keys, keys_partner), (projected, projected_partner)
    )
    keys_near, projected, sums = lax.optimization_barrier((keys_near, projected, sums))
    projected_near = exchange(projected, near_pairs)
    projected_far = exchange(projected, far_pairs)
    keys_over = exchange(keys_near, chip_pairs)
    shares_near, shares_far, shares_over, own_sum = attention_weights(
        counts, queries, (keys_near, keys_far, keys_over), sums, stats
    )
    projected_near, own_sum = lax.optimization_barrier((projected_near, own_sum))
    projected_over = exchange(projected_near, chip_pairs)
    most = gather((shares_near,), (projected_near,), own_sum)
    vel, squares = gather((shares_far, shares_over), (projected_far, projected_over), most, counts)

    squares = total_over(total_over(squares, Z_CORE), "blk_1")[0, 0]
    count = jnp.float32(LATENT_CH) * jnp.sum(valid.astype(jnp.float32))
    rms = jnp.sqrt(squares / count + 1e-06)
    velocity = vel / rms
    level = timestep[0].astype(jnp.float32)
    early = 1.0 - level / STEPS
    later = 1.0 - (level + 1.0) / STEPS
    sigma_early = 5.0 * early / (1.0 + 4.0 * early)
    sigma_later = 5.0 * later / (1.0 + 4.0 * later)
    return (velocity, latent + (sigma_later - sigma_early) * velocity)


def solution(mesh):
    split = Mesh(
        mesh.devices.reshape(mesh.shape["groups"], 16, 4, 2), ("groups", "blk_0", "blk_1", "blk_2")
    )
    return jax.shard_map(
        step,
        mesh=split,
        in_specs=(
            P(GROUPS_BLK, None),
            P(GROUPS_BLK, None),
            P(GROUPS_BLK, None),
            P(),
            P(None, GROUPS_BLK),
            P("groups"),
            P("groups"),
        ),
        out_specs=(P(None, GROUPS_BLK), P(None, GROUPS_BLK)),
        check_vma=False,
    )
```

```python
import functools
import math

import jax
import jax.numpy as jnp
from jax import lax
from jax.experimental import pallas as pl
from jax.experimental.pallas import tpu as pltpu
from jax.sharding import Mesh
from jax.sharding import PartitionSpec as P


HEADS = 20
HEAD_DIM = 128
LATENT_CH = 64
PAIRS = HEADS // 2
LANES = 2 * LATENT_CH
STEPS = 10
Z_CORE = ("blk_0", "blk_2")
BLK = ("blk_0", "blk_1", "blk_2")
GROUPS_BLK = ("groups", "blk_0", "blk_1", "blk_2")
SCORE_SCALE = math.log2(math.e) / math.sqrt(HEAD_DIM)
LARGEST = 3.3e38


def dot_last(left, right):
    return lax.dot_general(
        left, right, (((1,), (1,)), ((), ())), preferred_element_type=jnp.float32
    )


def dot_plain(left, right):
    return jnp.dot(left, right, preferred_element_type=jnp.float32)


def columns_of(pair, width):
    return pl.ds(pl.multiple_of(pair * width, width), width)


def project_kernel(counts, values, weight, out):
    def one_pair(pair, carry):
        held = values[:, columns_of(pair, 2 * HEAD_DIM)]
        used = lax.broadcasted_iota(jnp.int32, held.shape, 0) < counts[0]
        held = jnp.where(used, held, jnp.zeros_like(held))
        part = weight[:, columns_of(pair, 2 * HEAD_DIM)]
        even = lax.broadcasted_iota(jnp.int32, part.shape, 1) < HEAD_DIM
        zero = jnp.zeros_like(part)
        stacked = jnp.concatenate(
            [jnp.where(even, part, zero), jnp.where(even, zero, part)], axis=0
        )
        projected = jnp.clip(dot_last(held, stacked), -LARGEST, LARGEST)
        out[:, columns_of(pair, LANES)] = projected.astype(jnp.bfloat16)
        return carry

    lax.fori_loop(0, PAIRS, one_pair, 0)


def head_scores(query, keys, pair, side, columns, counts):
    pieces = []
    part = pl.ds(pl.multiple_of(pair * 2 * HEAD_DIM, HEAD_DIM) + side * HEAD_DIM, HEAD_DIM)
    for block, count in zip(keys, counts):
        score = dot_last(query[:, part], block[:, part]) * SCORE_SCALE
        for at in range(0, score.shape[1], LANES):
            piece = score[:, at : at + LANES]
            pieces.append(jnp.where(columns < count - at, piece, jnp.float32(-1e30)))
    return pieces


def row_max(pieces):
    top = jnp.max(functools.reduce(jnp.maximum, pieces), axis=-1, keepdims=True)
    return jnp.broadcast_to(top, pieces[0].shape)


def row_sum(pieces):
    total = jnp.sum(functools.reduce(jnp.add, pieces), axis=-1, keepdims=True)
    return jnp.broadcast_to(total, pieces[0].shape)


def own_kernel(counts, queries, *refs):
    keys, projected = refs[:2], refs[2:4]
    sums, tops, totals = refs[4:]
    rows = queries.shape[0]
    columns = lax.broadcasted_iota(jnp.int32, (rows, LANES), 1)
    block_counts = [counts[block] for block in range(2)]

    def one_pair(pair, carry):
        parts = []
        for side in range(2):
            pieces = head_scores(queries, keys, pair, side, columns, block_counts)
            top = row_max(pieces)
            weights = [jnp.exp2(piece - top) for piece in pieces]
            tops[2 * pair + side] = top
            totals[2 * pair + side] = row_sum(weights)
            rounded = [weight.astype(jnp.bfloat16) for weight in weights]
            half = len(rounded) // 2
            parts.append(
                dot_plain(
                    jnp.concatenate(rounded[:half], axis=1), projected[0][:, columns_of(pair, LANES)]
                )
                + dot_plain(
                    jnp.concatenate(rounded[half:], axis=1), projected[1][:, columns_of(pair, LANES)]
                )
            )
        sums[:, columns_of(pair, LANES)] = jnp.where(columns < LATENT_CH, *parts)
        return carry

    lax.fori_loop(0, PAIRS, one_pair, 0)


def weights_kernel(counts, queries, *refs):
    keys, (sums, tops, totals) = refs[:3], refs[3:6]
    remote, own_sum = refs[6:9], refs[9]
    rows = queries.shape[0]
    columns = lax.broadcasted_iota(jnp.int32, (rows, LANES), 1)
    block_counts = [counts[2 + block] for block in range(3)]
    own_sum[...] = jnp.zeros_like(own_sum)

    def one_pair(pair, carry):
        scales = []
        for side in range(2):
            pieces = head_scores(queries, keys, pair, side, columns, block_counts)
            own_top = tops[2 * pair + side]
            top = jnp.maximum(row_max(pieces), own_top)
            shrink = jnp.exp2(own_top - top)
            weights = [jnp.exp2(piece - top) for piece in pieces]
            share = 1.0 / (row_sum(weights) + totals[2 * pair + side] * shrink)
            per_block = len(weights) // len(remote)
            for at, weight in enumerate(weights):
                block, half = divmod(at, per_block)
                remote[block][2 * pair + side, :, half * LANES : (half + 1) * LANES] = (
                    weight * share
                ).astype(jnp.bfloat16)
            scales.append(shrink * share)
        scale = jnp.where(columns < LATENT_CH, *scales)
        own_sum[...] += sums[:, columns_of(pair, LANES)] * scale
        return carry

    lax.fori_loop(0, PAIRS, one_pair, 0)


def gather_kernel(blocks, finish, *refs):
    shares, values = refs[:blocks], refs[blocks : 2 * blocks]
    start = refs[2 * blocks]
    even_sum = jnp.zeros(start.shape, jnp.float32)
    odd_sum = jnp.zeros(start.shape, jnp.float32)
    for pair in range(PAIRS):
        for block in range(blocks):
            value = values[block][:, pair * LANES : (pair + 1) * LANES]
            even_sum += dot_plain(shares[block][2 * pair], value)
            odd_sum += dot_plain(shares[block][2 * pair + 1], value)
    low = lax.broadcasted_iota(jnp.int32, start.shape, 1) < LATENT_CH
    both = start[...] + jnp.where(low, even_sum, odd_sum)
    if not finish:
        refs[-1][...] = both
        return
    counts, out, squares = refs[-3:]
    both = both + pltpu.roll(both, LATENT_CH, 1)
    vel = jnp.transpose(both)[:LATENT_CH]
    used = lax.broadcasted_iota(jnp.int32, vel.shape, 1) < counts[0]
    vel = jnp.where(used, vel, 0.0)
    out[...] = vel
    square = jnp.sum(vel * vel, axis=0, keepdims=True)
    squares[...] = jnp.broadcast_to(jnp.sum(square, axis=1, keepdims=True), squares.shape)


def call(kernel, counts_first, operands, outs, limit=24):
    here = pl.BlockSpec(memory_space=pltpu.VMEM)
    scalars = pl.BlockSpec(memory_space=pltpu.SMEM)
    operands = [
        x if at == counts_first else pltpu.with_memory_space_constraint(x, pltpu.VMEM)
        for at, x in enumerate(operands)
    ]
    return pl.pallas_call(
        kernel,
        in_specs=[scalars if at == counts_first else here for at in range(len(operands))],
        out_specs=[here] * len(outs),
        out_shape=[pltpu.VMEM(shape, dtype) for shape, dtype in outs],
        compiler_params=pltpu.CompilerParams(vmem_limit_bytes=limit << 20),
    )(*operands)


def project(counts, values, weight):
    rows = values.shape[0]
    outs = [((rows, PAIRS * LANES), jnp.bfloat16)]
    return call(project_kernel, 0, (counts, values, weight), outs)[0]


def own_attention(counts, queries, keys, projected):
    rows = queries.shape[0]
    outs = [((rows, PAIRS * LANES), jnp.float32)] + [((HEADS, rows, LANES), jnp.float32)] * 2
    return call(own_kernel, 0, (counts, queries, *keys, *projected), outs)


def attention_weights(counts, queries, keys, own):
    rows = queries.shape[0]
    outs = [((HEADS, rows, rows), jnp.bfloat16)] * 3 + [((rows, LANES), jnp.float32)]
    return call(weights_kernel, 0, (counts, queries, *keys, *own), outs)


def gather(shares, values, start, counts=None, copies=1):
    rows = start.shape[0]
    blocks = len(shares)
    operands = [*shares, *values, start]
    if counts is None:
        kernel = functools.partial(gather_kernel, blocks, False)
        return call(kernel, -1, operands, [((rows, LANES), jnp.float32)])[0]
    kernel = functools.partial(gather_kernel, blocks, True)
    outs = [((LATENT_CH, rows), jnp.float32), ((copies, LANES), jnp.float32)]
    return call(kernel, len(operands), [*operands, counts], outs)


def exchange(shard, pairs):
    return lax.ppermute(shard, BLK, pairs)


def exchanged_sum(copies, axes):
    gathered = lax.all_to_all(copies, axes, 0, 0, tiled=True)
    return jnp.sum(gathered, axis=0, keepdims=True)


def step(queries, keys, values, out_weight, latent, valid, timestep):
    blocks = lax.axis_size(BLK)
    own = lax.axis_index(BLK)
    near_pairs = [((i + 2) % blocks if i % 2 == 0 else (i - 2) % blocks, i) for i in range(blocks)]
    far_pairs = [((i - 2) % blocks if i % 2 == 0 else (i + 2) % blocks, i) for i in range(blocks)]
    chip_pairs = [(i, i ^ 1) for i in range(blocks)]
    is_odd = own % 2
    partner = own + 1 - 2 * is_odd
    near = own + 2 - 4 * is_odd
    far = own - 2 + 4 * is_odd
    over = own - 1 + 2 * is_odd
    index = jnp.stack([own, partner, near, far, over])
    inside = (index >= 0) & (index < blocks)
    counts = jnp.where(inside, valid[jnp.clip(index, 0, blocks - 1)], 0).astype(jnp.int32)

    keys_near = exchange(keys, near_pairs)
    keys_far = exchange(keys, far_pairs)
    keys_partner = exchange(keys, chip_pairs)
    projected = project(counts, values, out_weight)
    projected_partner = exchange(projected, chip_pairs)
    own = own_attention(
        counts, queries, (keys, keys_partner), (projected, projected_partner)
    )
    keys_near, projected, *own = lax.optimization_barrier((keys_near, projected, *own))
    projected_near = exchange(projected, near_pairs)
    projected_far = exchange(projected, far_pairs)
    keys_over = exchange(keys_near, chip_pairs)
    shares_near, shares_far, shares_over, own_sum = attention_weights(
        counts, queries, (keys_near, keys_far, keys_over), own
    )
    projected_near, own_sum = lax.optimization_barrier((projected_near, own_sum))
    projected_over = exchange(projected_near, chip_pairs)
    most = gather((shares_near,), (projected_near,), own_sum)
    vel, squares = gather(
        (shares_far, shares_over),
        (projected_far, projected_over),
        most,
        counts,
        lax.axis_size(Z_CORE),
    )

    squares = exchanged_sum(squares, Z_CORE)
    copies = jnp.broadcast_to(squares, (lax.axis_size("blk_1"), LANES))
    squares = exchanged_sum(copies, "blk_1")[0, 0]
    count = jnp.float32(LATENT_CH) * jnp.sum(valid.astype(jnp.float32))
    rms = jnp.sqrt(squares / count + 1e-06)
    velocity = vel / rms
    level = timestep[0].astype(jnp.float32)
    early = 1.0 - level / STEPS
    later = 1.0 - (level + 1.0) / STEPS
    sigma_early = 5.0 * early / (1.0 + 4.0 * early)
    sigma_later = 5.0 * later / (1.0 + 4.0 * later)
    return (velocity, latent + (sigma_later - sigma_early) * velocity)


def solution(mesh):
    split = Mesh(
        mesh.devices.reshape(mesh.shape["groups"], 16, 4, 2), ("groups", "blk_0", "blk_1", "blk_2")
    )
    return jax.shard_map(
        step,
        mesh=split,
        in_specs=(
            P(GROUPS_BLK, None),
            P(GROUPS_BLK, None),
            P(GROUPS_BLK, None),
            P(),
            P(None, GROUPS_BLK),
            P("groups"),
            P("groups"),
        ),
        out_specs=(P(None, GROUPS_BLK), P(None, GROUPS_BLK)),
        check_vma=False,
    )
```

```python
import functools
import math

import jax
import jax.numpy as jnp
from jax import lax
from jax.experimental import pallas as pl
from jax.experimental.pallas import tpu as pltpu
from jax.sharding import Mesh
from jax.sharding import PartitionSpec as P


HEADS = 20
HEAD_DIM = 128
LATENT_CH = 64
PAIRS = HEADS // 2
LANES = 2 * LATENT_CH
STEPS = 10
Z_CORE = ("blk_0", "blk_2")
BLK = ("blk_0", "blk_1", "blk_2")
GROUPS_BLK = ("groups", "blk_0", "blk_1", "blk_2")
SCORE_SCALE = math.log2(math.e) / math.sqrt(HEAD_DIM)
LARGEST = 3.3e38


def dot_last(left, right):
    return lax.dot_general(
        left, right, (((1,), (1,)), ((), ())), preferred_element_type=jnp.float32
    )


def dot_plain(left, right):
    return jnp.dot(left, right, preferred_element_type=jnp.float32)


def columns_of(pair, width):
    return pl.ds(pl.multiple_of(pair * width, width), width)


def project_kernel(counts, values, weight, out):
    def one_pair(pair, carry):
        held = values[:, columns_of(pair, 2 * HEAD_DIM)]
        used = lax.broadcasted_iota(jnp.int32, held.shape, 0) < counts[0]
        held = jnp.where(used, held, jnp.zeros_like(held))
        part = weight[:, columns_of(pair, 2 * HEAD_DIM)]
        even = lax.broadcasted_iota(jnp.int32, part.shape, 1) < HEAD_DIM
        zero = jnp.zeros_like(part)
        stacked = jnp.concatenate(
            [jnp.where(even, part, zero), jnp.where(even, zero, part)], axis=0
        )
        projected = jnp.clip(dot_last(held, stacked), -LARGEST, LARGEST)
        out[:, columns_of(pair, LANES)] = projected.astype(jnp.bfloat16)
        return carry

    lax.fori_loop(0, PAIRS, one_pair, 0)


def head_scores(query, keys, pair, side, columns, counts):
    pieces = []
    part = pl.ds(pl.multiple_of(pair * 2 * HEAD_DIM, HEAD_DIM) + side * HEAD_DIM, HEAD_DIM)
    for block, count in zip(keys, counts):
        score = dot_last(query[:, part], block[:, part]) * SCORE_SCALE
        for at in range(0, score.shape[1], LANES):
            piece = score[:, at : at + LANES]
            pieces.append(jnp.where(columns < count - at, piece, jnp.float32(-1e30)))
    return pieces


def row_max(pieces):
    top = jnp.max(functools.reduce(jnp.maximum, pieces), axis=-1, keepdims=True)
    return jnp.broadcast_to(top, pieces[0].shape)


def row_sum(pieces):
    total = jnp.sum(functools.reduce(jnp.add, pieces), axis=-1, keepdims=True)
    return jnp.broadcast_to(total, pieces[0].shape)


def own_kernel(counts, queries, *refs):
    keys, projected = refs[:2], refs[2:4]
    sums, tops, totals = refs[4:]
    rows = queries.shape[0]
    columns = lax.broadcasted_iota(jnp.int32, (rows, LANES), 1)
    block_counts = [counts[block] for block in range(2)]

    def one_pair(pair, carry):
        parts = []
        for side in range(2):
            pieces = head_scores(queries, keys, pair, side, columns, block_counts)
            top = row_max(pieces)
            weights = [jnp.exp2(piece - top) for piece in pieces]
            tops[2 * pair + side] = top
            totals[2 * pair + side] = row_sum(weights)
            rounded = [weight.astype(jnp.bfloat16) for weight in weights]
            half = len(rounded) // 2
            parts.append(
                dot_plain(
                    jnp.concatenate(rounded[:half], axis=1), projected[0][:, columns_of(pair, LANES)]
                )
                + dot_plain(
                    jnp.concatenate(rounded[half:], axis=1), projected[1][:, columns_of(pair, LANES)]
                )
            )
        sums[:, columns_of(pair, LANES)] = jnp.where(columns < LATENT_CH, *parts)
        return carry

    lax.fori_loop(0, PAIRS, one_pair, 0)


def weights_kernel(counts, queries, *refs):
    keys, (sums, tops, totals) = refs[:3], refs[3:6]
    remote, own_sum = refs[6:9], refs[9]
    rows = queries.shape[0]
    columns = lax.broadcasted_iota(jnp.int32, (rows, LANES), 1)
    block_counts = [counts[2 + block] for block in range(3)]
    own_sum[...] = jnp.zeros_like(own_sum)

    def one_pair(pair, carry):
        scales = []
        for side in range(2):
            pieces = head_scores(queries, keys, pair, side, columns, block_counts)
            own_top = tops[2 * pair + side]
            top = jnp.maximum(row_max(pieces), own_top)
            shrink = jnp.exp2(own_top - top)
            weights = [jnp.exp2(piece - top) for piece in pieces]
            share = 1.0 / (row_sum(weights) + totals[2 * pair + side] * shrink)
            per_block = len(weights) // len(remote)
            for at, weight in enumerate(weights):
                block, half = divmod(at, per_block)
                remote[block][2 * pair + side, :, half * LANES : (half + 1) * LANES] = (
                    weight * share
                ).astype(jnp.bfloat16)
            scales.append(shrink * share)
        scale = jnp.where(columns < LATENT_CH, *scales)
        own_sum[...] += sums[:, columns_of(pair, LANES)] * scale
        return carry

    lax.fori_loop(0, PAIRS, one_pair, 0)


def gather_kernel(blocks, finish, *refs):
    shares, values = refs[:blocks], refs[blocks : 2 * blocks]
    start = refs[2 * blocks]
    even_sum = jnp.zeros(start.shape, jnp.float32)
    odd_sum = jnp.zeros(start.shape, jnp.float32)
    for pair in range(PAIRS):
        for block in range(blocks):
            value = values[block][:, pair * LANES : (pair + 1) * LANES]
            even_sum += dot_plain(shares[block][2 * pair], value)
            odd_sum += dot_plain(shares[block][2 * pair + 1], value)
    low = lax.broadcasted_iota(jnp.int32, start.shape, 1) < LATENT_CH
    both = start[...] + jnp.where(low, even_sum, odd_sum)
    if not finish:
        refs[-1][...] = both
        return
    counts, out, squares = refs[-3:]
    both = both + pltpu.roll(both, LATENT_CH, 1)
    vel = jnp.transpose(both)[:LATENT_CH]
    used = lax.broadcasted_iota(jnp.int32, vel.shape, 1) < counts[0]
    vel = jnp.where(used, vel, 0.0)
    out[...] = vel
    square = jnp.sum(vel * vel, axis=0, keepdims=True)
    squares[...] = jnp.broadcast_to(jnp.sum(square, axis=1, keepdims=True), squares.shape)


def call(kernel, counts_first, operands, outs, limit=24):
    here = pl.BlockSpec(memory_space=pltpu.VMEM)
    scalars = pl.BlockSpec(memory_space=pltpu.SMEM)
    operands = [
        x if at == counts_first else pltpu.with_memory_space_constraint(x, pltpu.VMEM)
        for at, x in enumerate(operands)
    ]
    return pl.pallas_call(
        kernel,
        in_specs=[scalars if at == counts_first else here for at in range(len(operands))],
        out_specs=[here] * len(outs),
        out_shape=[pltpu.VMEM(shape, dtype) for shape, dtype in outs],
        compiler_params=pltpu.CompilerParams(vmem_limit_bytes=limit << 20),
    )(*operands)


def project(counts, values, weight):
    rows = values.shape[0]
    outs = [((rows, PAIRS * LANES), jnp.bfloat16)]
    return call(project_kernel, 0, (counts, values, weight), outs)[0]


def own_attention(counts, queries, keys, projected):
    rows = queries.shape[0]
    outs = [((rows, PAIRS * LANES), jnp.float32)] + [((HEADS, rows, LANES), jnp.float32)] * 2
    return call(own_kernel, 0, (counts, queries, *keys, *projected), outs)


def attention_weights(counts, queries, keys, own):
    rows = queries.shape[0]
    outs = [((HEADS, rows, rows), jnp.bfloat16)] * 3 + [((rows, LANES), jnp.float32)]
    return call(weights_kernel, 0, (counts, queries, *keys, *own), outs)


def gather(shares, values, start, counts=None, copies=1):
    rows = start.shape[0]
    blocks = len(shares)
    operands = [*shares, *values, start]
    if counts is None:
        kernel = functools.partial(gather_kernel, blocks, False)
        return call(kernel, -1, operands, [((rows, LANES), jnp.float32)])[0]
    kernel = functools.partial(gather_kernel, blocks, True)
    outs = [((LATENT_CH, rows), jnp.float32), ((copies, LANES), jnp.float32)]
    return call(kernel, len(operands), [*operands, counts], outs)


def exchange(shard, pairs):
    return lax.ppermute(shard, BLK, pairs)


def exchanged_sum(copies, axes):
    gathered = lax.all_to_all(copies, axes, 0, 0, tiled=True)
    return jnp.sum(gathered, axis=0, keepdims=True)


def step(queries, keys, values, out_weight, latent, valid, timestep):
    blocks = lax.axis_size(BLK)
    own = lax.axis_index(BLK)
    near_pairs = [((i + 2) % blocks if i % 2 == 0 else (i - 2) % blocks, i) for i in range(blocks)]
    far_pairs = [((i - 2) % blocks if i % 2 == 0 else (i + 2) % blocks, i) for i in range(blocks)]
    chip_pairs = [(i, i ^ 1) for i in range(blocks)]
    is_odd = own % 2
    partner = own + 1 - 2 * is_odd
    near = own + 2 - 4 * is_odd
    far = own - 2 + 4 * is_odd
    over = own - 1 + 2 * is_odd
    index = jnp.stack([own, partner, near, far, over])
    inside = (index >= 0) & (index < blocks)
    counts = jnp.where(inside, valid[jnp.clip(index, 0, blocks - 1)], 0).astype(jnp.int32)

    keys_near = exchange(keys, near_pairs)
    keys_far = exchange(keys, far_pairs)
    keys_partner = exchange(keys, chip_pairs)
    projected = project(counts, values, out_weight)
    projected_partner = exchange(projected, chip_pairs)
    own = own_attention(
        counts, queries, (keys, keys_partner), (projected, projected_partner)
    )
    projected, *own = lax.optimization_barrier((projected, *own))
    projected_near = exchange(projected, near_pairs)
    projected_far = exchange(projected, far_pairs)
    keys_over = exchange(keys_near, chip_pairs)
    shares_near, shares_far, shares_over, own_sum = attention_weights(
        counts, queries, (keys_near, keys_far, keys_over), own
    )
    projected_near, own_sum = lax.optimization_barrier((projected_near, own_sum))
    projected_over = exchange(projected_near, chip_pairs)
    most = gather((shares_near,), (projected_near,), own_sum)
    most = gather((shares_far,), (projected_far,), most)
    vel, squares = gather(
        (shares_over,),
        (projected_over,),
        most,
        counts,
        1,
    )

    columns = lax.axis_size("blk_1")
    moved = [
        lax.ppermute(squares, "blk_1", [(i, (i + by) % columns) for i in range(columns)])
        for by in range(1, columns)
    ]
    squares = functools.reduce(jnp.add, moved, squares)
    copies = jnp.broadcast_to(squares, (lax.axis_size(Z_CORE), LANES))
    squares = exchanged_sum(copies, Z_CORE)[0, 0]
    count = jnp.float32(LATENT_CH) * jnp.sum(valid.astype(jnp.float32))
    rms = jnp.sqrt(squares / count + 1e-06)
    velocity = vel / rms
    level = timestep[0].astype(jnp.float32)
    early = 1.0 - level / STEPS
    later = 1.0 - (level + 1.0) / STEPS
    sigma_early = 5.0 * early / (1.0 + 4.0 * early)
    sigma_later = 5.0 * later / (1.0 + 4.0 * later)
    return (velocity, latent + (sigma_later - sigma_early) * velocity)


def solution(mesh):
    split = Mesh(
        mesh.devices.reshape(mesh.shape["groups"], 16, 4, 2), ("groups", "blk_0", "blk_1", "blk_2")
    )
    return jax.shard_map(
        step,
        mesh=split,
        in_specs=(
            P(GROUPS_BLK, None),
            P(GROUPS_BLK, None),
            P(GROUPS_BLK, None),
            P(),
            P(None, GROUPS_BLK),
            P("groups"),
            P("groups"),
        ),
        out_specs=(P(None, GROUPS_BLK), P(None, GROUPS_BLK)),
        check_vma=False,
    )
```

```python
import functools
import math

import jax
import jax.numpy as jnp
from jax import lax
from jax.experimental import pallas as pl
from jax.experimental.pallas import tpu as pltpu
from jax.sharding import Mesh
from jax.sharding import PartitionSpec as P


HEADS = 20
HEAD_DIM = 128
LATENT_CH = 64
PAIRS = HEADS // 2
LANES = 2 * LATENT_CH
OWN, _, NEAR, FAR, OVER = range(5)
STEPS = 10
Z_CORE = ("blk_0", "blk_2")
BLK = ("blk_0", "blk_1", "blk_2")
GROUPS_BLK = ("groups", "blk_0", "blk_1", "blk_2")
SCORE_SCALE = math.log2(math.e) / math.sqrt(HEAD_DIM)
LARGEST = 3.3e38


def dot_last(left, right):
    return lax.dot_general(
        left, right, (((1,), (1,)), ((), ())), preferred_element_type=jnp.float32
    )


def dot_plain(left, right):
    return jnp.dot(left, right, preferred_element_type=jnp.float32)


def columns_of(pair, width):
    return pl.ds(pl.multiple_of(pair * width, width), width)


def project_kernel(counts, values, weight, out):
    def one_pair(pair, carry):
        held = values[:, columns_of(pair, 2 * HEAD_DIM)]
        used = lax.broadcasted_iota(jnp.int32, held.shape, 0) < counts[0]
        held = jnp.where(used, held, jnp.zeros_like(held))
        part = weight[:, columns_of(pair, 2 * HEAD_DIM)]
        even = lax.broadcasted_iota(jnp.int32, part.shape, 1) < HEAD_DIM
        zero = jnp.zeros_like(part)
        stacked = jnp.concatenate(
            [jnp.where(even, part, zero), jnp.where(even, zero, part)], axis=0
        )
        projected = jnp.clip(dot_last(held, stacked), -LARGEST, LARGEST)
        out[:, columns_of(pair, LANES)] = projected.astype(jnp.bfloat16)
        return carry

    lax.fori_loop(0, PAIRS, one_pair, 0)


def head_scores(query, keys, pair, side, columns, counts):
    pieces = []
    part = pl.ds(pl.multiple_of(pair * 2 * HEAD_DIM, HEAD_DIM) + side * HEAD_DIM, HEAD_DIM)
    for block, count in zip(keys, counts):
        score = dot_last(query[:, part], block[:, part]) * SCORE_SCALE
        for at in range(0, score.shape[1], LANES):
            piece = score[:, at : at + LANES]
            pieces.append(jnp.where(columns < count - at, piece, jnp.float32(-1e30)))
    return pieces


def row_max(pieces):
    top = jnp.max(functools.reduce(jnp.maximum, pieces), axis=-1, keepdims=True)
    return jnp.broadcast_to(top, pieces[0].shape)


def row_sum(pieces):
    total = jnp.sum(functools.reduce(jnp.add, pieces), axis=-1, keepdims=True)
    return jnp.broadcast_to(total, pieces[0].shape)


def own_kernel(counts, queries, *refs):
    keys, projected = refs[:2], refs[2:4]
    sums, tops, totals = refs[4:]
    rows = queries.shape[0]
    columns = lax.broadcasted_iota(jnp.int32, (rows, LANES), 1)
    block_counts = [counts[block] for block in range(2)]

    def one_pair(pair, carry):
        parts = []
        for side in range(2):
            pieces = head_scores(queries, keys, pair, side, columns, block_counts)
            top = row_max(pieces)
            weights = [jnp.exp2(piece - top) for piece in pieces]
            tops[2 * pair + side] = top
            totals[2 * pair + side] = row_sum(weights)
            rounded = [weight.astype(jnp.bfloat16) for weight in weights]
            half = len(rounded) // 2
            parts.append(
                dot_plain(
                    jnp.concatenate(rounded[:half], axis=1), projected[0][:, columns_of(pair, LANES)]
                )
                + dot_plain(
                    jnp.concatenate(rounded[half:], axis=1), projected[1][:, columns_of(pair, LANES)]
                )
            )
        sums[:, columns_of(pair, LANES)] = jnp.where(columns < LATENT_CH, *parts)
        return carry

    lax.fori_loop(0, PAIRS, one_pair, 0)


def merge_kernel(counts, queries, *refs):
    keys, (sums, tops, totals) = refs[:2], refs[2:5]
    near, over, new_sums, new_tops, new_totals = refs[5:]
    rows = queries.shape[0]
    columns = lax.broadcasted_iota(jnp.int32, (rows, LANES), 1)
    block_counts = [counts[NEAR], counts[OVER]]

    def one_pair(pair, carry):
        shrinks = []
        for side in range(2):
            head = 2 * pair + side
            pieces = head_scores(queries, keys, pair, side, columns, block_counts)
            own_top = tops[head]
            top = jnp.maximum(row_max(pieces), own_top)
            shrink = jnp.exp2(own_top - top)
            weights = [jnp.exp2(piece - top) for piece in pieces]
            new_tops[head] = top
            new_totals[head] = row_sum(weights) + totals[head] * shrink
            per_block = len(weights) // 2
            for at, weight in enumerate(weights):
                block, half = divmod(at, per_block)
                (near, over)[block][head, :, half * LANES : (half + 1) * LANES] = weight.astype(
                    jnp.bfloat16
                )
            shrinks.append(shrink)
        shrink = jnp.where(columns < LATENT_CH, *shrinks)
        new_sums[:, columns_of(pair, LANES)] = sums[:, columns_of(pair, LANES)] * shrink
        return carry

    lax.fori_loop(0, PAIRS, one_pair, 0)


def collect_kernel(near, over, near_values, over_values, sums, scales, out):
    low = lax.broadcasted_iota(jnp.int32, out.shape, 1) < LATENT_CH
    total = jnp.zeros(out.shape, jnp.float32)
    for pair in range(PAIRS):
        lanes = slice(pair * LANES, (pair + 1) * LANES)
        even, odd = [
            dot_plain(near[head], near_values[:, lanes])
            + dot_plain(over[head], over_values[:, lanes])
            for head in (2 * pair, 2 * pair + 1)
        ]
        total += (sums[:, lanes] + jnp.where(low, even, odd)) * scales[pair]
    out[...] = total


def weights_kernel(counts, queries, keys, tops, totals, shares, scales):
    rows = queries.shape[0]
    columns = lax.broadcasted_iota(jnp.int32, (rows, LANES), 1)
    block_counts = [counts[FAR]]

    def one_pair(pair, carry):
        factors = []
        for side in range(2):
            head = 2 * pair + side
            pieces = head_scores(queries, [keys], pair, side, columns, block_counts)
            old_top = tops[head]
            top = jnp.maximum(row_max(pieces), old_top)
            shrink = jnp.exp2(old_top - top)
            weights = [jnp.exp2(piece - top) for piece in pieces]
            share = 1.0 / (row_sum(weights) + totals[head] * shrink)
            for half, weight in enumerate(weights):
                shares[head, :, half * LANES : (half + 1) * LANES] = (weight * share).astype(
                    jnp.bfloat16
                )
            factors.append(shrink * share)
        scales[pair] = jnp.where(columns < LATENT_CH, *factors)
        return carry

    lax.fori_loop(0, PAIRS, one_pair, 0)


def finish_kernel(shares, values, most, counts, out, squares):
    even_sum = jnp.zeros(most.shape, jnp.float32)
    odd_sum = jnp.zeros(most.shape, jnp.float32)
    for pair in range(PAIRS):
        value = values[:, pair * LANES : (pair + 1) * LANES]
        even_sum += dot_plain(shares[2 * pair], value)
        odd_sum += dot_plain(shares[2 * pair + 1], value)
    low = lax.broadcasted_iota(jnp.int32, most.shape, 1) < LATENT_CH
    both = most[...] + jnp.where(low, even_sum, odd_sum)
    both = both + pltpu.roll(both, LATENT_CH, 1)
    vel = jnp.transpose(both)[:LATENT_CH]
    used = lax.broadcasted_iota(jnp.int32, vel.shape, 1) < counts[OWN]
    vel = jnp.where(used, vel, 0.0)
    out[...] = vel
    square = jnp.sum(vel * vel, axis=0, keepdims=True)
    squares[...] = jnp.broadcast_to(jnp.sum(square, axis=1, keepdims=True), squares.shape)


def call(kernel, counts_first, operands, outs, limit=24):
    here = pl.BlockSpec(memory_space=pltpu.VMEM)
    scalars = pl.BlockSpec(memory_space=pltpu.SMEM)
    operands = [
        x if at == counts_first else pltpu.with_memory_space_constraint(x, pltpu.VMEM)
        for at, x in enumerate(operands)
    ]
    return pl.pallas_call(
        kernel,
        in_specs=[scalars if at == counts_first else here for at in range(len(operands))],
        out_specs=[here] * len(outs),
        out_shape=[pltpu.VMEM(shape, dtype) for shape, dtype in outs],
        compiler_params=pltpu.CompilerParams(vmem_limit_bytes=limit << 20),
    )(*operands)


def project(counts, values, weight):
    rows = values.shape[0]
    outs = [((rows, PAIRS * LANES), jnp.bfloat16)]
    return call(project_kernel, 0, (counts, values, weight), outs)[0]


def own_attention(counts, queries, keys, projected):
    rows = queries.shape[0]
    outs = [((rows, PAIRS * LANES), jnp.float32)] + [((HEADS, rows, LANES), jnp.float32)] * 2
    return call(own_kernel, 0, (counts, queries, *keys, *projected), outs)


def merge(counts, queries, keys, own):
    rows = queries.shape[0]
    outs = [((HEADS, rows, rows), jnp.bfloat16)] * 2 + [((rows, PAIRS * LANES), jnp.float32)]
    outs += [((HEADS, rows, LANES), jnp.float32)] * 2
    return call(merge_kernel, 0, (counts, queries, *keys, *own), outs)


def collect(weights, values, sums, scales):
    outs = [((sums.shape[0], LANES), jnp.float32)]
    return call(collect_kernel, -1, (*weights, *values, sums, scales), outs)[0]


def last_weights(counts, queries, keys, tops, totals):
    rows = queries.shape[0]
    outs = [((HEADS, rows, rows), jnp.bfloat16), ((PAIRS, rows, LANES), jnp.float32)]
    return call(weights_kernel, 0, (counts, queries, keys, tops, totals), outs)


def finish(shares, values, most, counts):
    outs = [((LATENT_CH, most.shape[0]), jnp.float32), ((1, LANES), jnp.float32)]
    return call(finish_kernel, 3, (shares, values, most, counts), outs)


def exchange(shard, pairs):
    return lax.ppermute(shard, BLK, pairs)


def exchanged_sum(copies, axes):
    gathered = lax.all_to_all(copies, axes, 0, 0, tiled=True)
    return jnp.sum(gathered, axis=0, keepdims=True)


def step(queries, keys, values, out_weight, latent, valid, timestep):
    blocks = lax.axis_size(BLK)
    own = lax.axis_index(BLK)
    near_pairs = [((i + 2) % blocks if i % 2 == 0 else (i - 2) % blocks, i) for i in range(blocks)]
    far_pairs = [((i - 2) % blocks if i % 2 == 0 else (i + 2) % blocks, i) for i in range(blocks)]
    chip_pairs = [(i, i ^ 1) for i in range(blocks)]
    is_odd = own % 2
    partner = own + 1 - 2 * is_odd
    near = own + 2 - 4 * is_odd
    far = own - 2 + 4 * is_odd
    over = own - 1 + 2 * is_odd
    index = jnp.stack([own, partner, near, far, over])
    inside = (index >= 0) & (index < blocks)
    counts = jnp.where(inside, valid[jnp.clip(index, 0, blocks - 1)], 0).astype(jnp.int32)

    keys_near = exchange(keys, near_pairs)
    keys_far = exchange(keys, far_pairs)
    keys_partner = exchange(keys, chip_pairs)
    projected = project(counts, values, out_weight)
    projected_near = exchange(projected, near_pairs)
    projected_partner = exchange(projected, chip_pairs)
    own_sums, own_tops, own_totals = own_attention(
        counts, queries, (keys, keys_partner), (projected, projected_partner)
    )
    projected, own_sums = lax.optimization_barrier((projected, own_sums))
    projected_far = exchange(projected, far_pairs)
    keys_over = exchange(keys_near, chip_pairs)
    weights_near, weights_over, sums, tops, totals = merge(
        counts, queries, (keys_near, keys_over), (own_sums, own_tops, own_totals)
    )
    projected_near, sums = lax.optimization_barrier((projected_near, sums))
    projected_over = exchange(projected_near, chip_pairs)
    shares, scales = last_weights(counts, queries, keys_far, tops, totals)
    most = collect(
        (weights_near, weights_over), (projected_near, projected_over), sums, scales
    )
    vel, squares = finish(shares, projected_far, most, counts)

    columns = lax.axis_size("blk_1")
    moved = [
        lax.ppermute(squares, "blk_1", [(i, (i + by) % columns) for i in range(columns)])
        for by in range(1, columns)
    ]
    squares = functools.reduce(jnp.add, moved, squares)
    copies = jnp.broadcast_to(squares, (lax.axis_size(Z_CORE), LANES))
    squares = exchanged_sum(copies, Z_CORE)[0, 0]
    count = jnp.float32(LATENT_CH) * jnp.sum(valid.astype(jnp.float32))
    rms = jnp.sqrt(squares / count + 1e-06)
    velocity = vel / rms
    level = timestep[0].astype(jnp.float32)
    early = 1.0 - level / STEPS
    later = 1.0 - (level + 1.0) / STEPS
    sigma_early = 5.0 * early / (1.0 + 4.0 * early)
    sigma_later = 5.0 * later / (1.0 + 4.0 * later)
    return (velocity, latent + (sigma_later - sigma_early) * velocity)


def solution(mesh):
    split = Mesh(
        mesh.devices.reshape(mesh.shape["groups"], 16, 4, 2), ("groups", "blk_0", "blk_1", "blk_2")
    )
    return jax.shard_map(
        step,
        mesh=split,
        in_specs=(
            P(GROUPS_BLK, None),
            P(GROUPS_BLK, None),
            P(GROUPS_BLK, None),
            P(),
            P(None, GROUPS_BLK),
            P("groups"),
            P("groups"),
        ),
        out_specs=(P(None, GROUPS_BLK), P(None, GROUPS_BLK)),
        check_vma=False,
    )
```

```python
import functools
import math

import jax
import jax.numpy as jnp
from jax import lax
from jax.experimental import pallas as pl
from jax.experimental.pallas import tpu as pltpu
from jax.sharding import Mesh
from jax.sharding import PartitionSpec as P


HEADS = 20
HEAD_DIM = 128
LATENT_CH = 64
PAIRS = HEADS // 2
LANES = 2 * LATENT_CH
OWN, PARTNER, NEAR, FAR, OVER = range(5)
STEPS = 10
Z_CORE = ("blk_0", "blk_2")
BLK = ("blk_0", "blk_1", "blk_2")
GROUPS_BLK = ("groups", "blk_0", "blk_1", "blk_2")
SCORE_SCALE = math.log2(math.e) / math.sqrt(HEAD_DIM)
LARGEST = 3.3e38


def dot_last(left, right):
    return lax.dot_general(
        left, right, (((1,), (1,)), ((), ())), preferred_element_type=jnp.float32
    )


def dot_plain(left, right):
    return jnp.dot(left, right, preferred_element_type=jnp.float32)


def columns_of(pair, width):
    return pl.ds(pl.multiple_of(pair * width, width), width)


def project_kernel(counts, values, weight, out):
    def one_pair(pair, carry):
        held = values[:, columns_of(pair, 2 * HEAD_DIM)]
        used = lax.broadcasted_iota(jnp.int32, (held.shape[0], LANES), 0) < counts[OWN : OWN + 1, :]
        halves = [held[:, :LANES], held[:, LANES:]]
        held = jnp.concatenate([jnp.where(used, x, jnp.zeros_like(x)) for x in halves], axis=1)
        part = weight[:, columns_of(pair, 2 * HEAD_DIM)]
        even = lax.broadcasted_iota(jnp.int32, part.shape, 1) < HEAD_DIM
        zero = jnp.zeros_like(part)
        stacked = jnp.concatenate(
            [jnp.where(even, part, zero), jnp.where(even, zero, part)], axis=0
        )
        projected = jnp.clip(dot_last(held, stacked), -LARGEST, LARGEST)
        out[:, columns_of(pair, LANES)] = projected.astype(jnp.bfloat16)
        return carry

    lax.fori_loop(0, PAIRS, one_pair, 0)


def head_scores(query, keys, pair, side, columns, counts):
    pieces = []
    part = pl.ds(pl.multiple_of(pair * 2 * HEAD_DIM, HEAD_DIM) + side * HEAD_DIM, HEAD_DIM)
    for block, count in zip(keys, counts):
        score = dot_last(query[:, part], block[:, part]) * SCORE_SCALE
        for at in range(0, score.shape[1], LANES):
            piece = score[:, at : at + LANES]
            pieces.append(jnp.where(columns < count - at, piece, jnp.float32(-1e30)))
    return pieces


def row_max(pieces):
    top = jnp.max(functools.reduce(jnp.maximum, pieces), axis=-1, keepdims=True)
    return jnp.broadcast_to(top, pieces[0].shape)


def row_sum(pieces):
    total = jnp.sum(functools.reduce(jnp.add, pieces), axis=-1, keepdims=True)
    return jnp.broadcast_to(total, pieces[0].shape)


def own_kernel(counts, queries, *refs):
    keys, projected = refs[:2], refs[2:4]
    sums, tops, totals = refs[4:]
    rows = queries.shape[0]
    columns = lax.broadcasted_iota(jnp.int32, (rows, LANES), 1)
    block_counts = [counts[block : block + 1, :] for block in (OWN, PARTNER)]

    def one_pair(pair, carry):
        parts = []
        for side in range(2):
            pieces = head_scores(queries, keys, pair, side, columns, block_counts)
            top = row_max(pieces)
            weights = [jnp.exp2(piece - top) for piece in pieces]
            tops[2 * pair + side] = top
            totals[2 * pair + side] = row_sum(weights)
            rounded = [weight.astype(jnp.bfloat16) for weight in weights]
            half = len(rounded) // 2
            parts.append(
                dot_plain(
                    jnp.concatenate(rounded[:half], axis=1), projected[0][:, columns_of(pair, LANES)]
                )
                + dot_plain(
                    jnp.concatenate(rounded[half:], axis=1), projected[1][:, columns_of(pair, LANES)]
                )
            )
        sums[:, columns_of(pair, LANES)] = jnp.where(columns < LATENT_CH, *parts)
        return carry

    lax.fori_loop(0, PAIRS, one_pair, 0)


def merge_kernel(counts, queries, *refs):
    keys, (sums, tops, totals) = refs[:2], refs[2:5]
    near, over, new_sums, new_tops, new_totals = refs[5:]
    rows = queries.shape[0]
    columns = lax.broadcasted_iota(jnp.int32, (rows, LANES), 1)
    block_counts = [counts[block : block + 1, :] for block in (NEAR, OVER)]

    def one_pair(pair, carry):
        shrinks = []
        for side in range(2):
            head = 2 * pair + side
            pieces = head_scores(queries, keys, pair, side, columns, block_counts)
            own_top = tops[head]
            top = jnp.maximum(row_max(pieces), own_top)
            shrink = jnp.exp2(own_top - top)
            weights = [jnp.exp2(piece - top) for piece in pieces]
            new_tops[head] = top
            new_totals[head] = row_sum(weights) + totals[head] * shrink
            per_block = len(weights) // 2
            for at, weight in enumerate(weights):
                block, half = divmod(at, per_block)
                (near, over)[block][head, :, half * LANES : (half + 1) * LANES] = weight.astype(
                    jnp.bfloat16
                )
            shrinks.append(shrink)
        shrink = jnp.where(columns < LATENT_CH, *shrinks)
        new_sums[:, columns_of(pair, LANES)] = sums[:, columns_of(pair, LANES)] * shrink
        return carry

    lax.fori_loop(0, PAIRS, one_pair, 0)


def collect_kernel(near, over, near_values, over_values, sums, scales, out):
    low = lax.broadcasted_iota(jnp.int32, out.shape, 1) < LATENT_CH
    total = jnp.zeros(out.shape, jnp.float32)
    for pair in range(PAIRS):
        lanes = slice(pair * LANES, (pair + 1) * LANES)
        stacked = jnp.concatenate([near_values[:, lanes], over_values[:, lanes]], axis=0)
        even, odd = [
            dot_plain(jnp.concatenate([near[head], over[head]], axis=1), stacked)
            for head in (2 * pair, 2 * pair + 1)
        ]
        total += (sums[:, lanes] + jnp.where(low, even, odd)) * scales[pair]
    out[...] = total


def weights_kernel(counts, queries, keys, tops, totals, shares, scales):
    rows = queries.shape[0]
    columns = lax.broadcasted_iota(jnp.int32, (rows, LANES), 1)
    block_counts = [counts[FAR : FAR + 1, :]]

    def one_pair(pair, carry):
        factors = []
        for side in range(2):
            head = 2 * pair + side
            pieces = head_scores(queries, [keys], pair, side, columns, block_counts)
            old_top = tops[head]
            top = jnp.maximum(row_max(pieces), old_top)
            shrink = jnp.exp2(old_top - top)
            weights = [jnp.exp2(piece - top) for piece in pieces]
            share = 1.0 / (row_sum(weights) + totals[head] * shrink)
            for half, weight in enumerate(weights):
                shares[head, :, half * LANES : (half + 1) * LANES] = (weight * share).astype(
                    jnp.bfloat16
                )
            factors.append(shrink * share)
        scales[pair] = jnp.where(columns < LATENT_CH, *factors)
        return carry

    lax.fori_loop(0, PAIRS, one_pair, 0)


def finish_kernel(shares, values, most, counts, out, squares):
    stacked = jnp.concatenate(
        [values[:, pair * LANES : (pair + 1) * LANES] for pair in range(PAIRS)], axis=0
    )
    even_sum, odd_sum = [
        dot_plain(jnp.concatenate([shares[2 * pair + side] for pair in range(PAIRS)], axis=1), stacked)
        for side in range(2)
    ]
    low = lax.broadcasted_iota(jnp.int32, most.shape, 1) < LATENT_CH
    both = most[...] + jnp.where(low, even_sum, odd_sum)
    both = both + pltpu.roll(both, LATENT_CH, 1)
    used = lax.broadcasted_iota(jnp.int32, both.shape, 0) < counts[OWN : OWN + 1, :]
    vel = jnp.transpose(jnp.where(used, both, 0.0))[:LATENT_CH]
    out[...] = vel
    square = jnp.sum(vel * vel, axis=0, keepdims=True)
    squares[...] = jnp.broadcast_to(jnp.sum(square, axis=1, keepdims=True), squares.shape)


def call(kernel, operands, outs):
    here = pl.BlockSpec(memory_space=pltpu.VMEM)
    return pl.pallas_call(
        kernel,
        in_specs=[here] * len(operands),
        out_specs=[here] * len(outs),
        out_shape=[pltpu.VMEM(shape, dtype) for shape, dtype in outs],
        compiler_params=pltpu.CompilerParams(vmem_limit_bytes=24 << 20),
    )(*[pltpu.with_memory_space_constraint(x, pltpu.VMEM) for x in operands])


def project(counts, values, weight):
    rows = values.shape[0]
    outs = [((rows, PAIRS * LANES), jnp.bfloat16)]
    return call(project_kernel, (counts, values, weight), outs)[0]


def own_attention(counts, queries, keys, projected):
    rows = queries.shape[0]
    outs = [((rows, PAIRS * LANES), jnp.float32)] + [((HEADS, rows, LANES), jnp.float32)] * 2
    return call(own_kernel, (counts, queries, *keys, *projected), outs)


def merge(counts, queries, keys, own):
    rows = queries.shape[0]
    outs = [((HEADS, rows, rows), jnp.bfloat16)] * 2 + [((rows, PAIRS * LANES), jnp.float32)]
    outs += [((HEADS, rows, LANES), jnp.float32)] * 2
    return call(merge_kernel, (counts, queries, *keys, *own), outs)


def collect(weights, values, sums, scales):
    outs = [((sums.shape[0], LANES), jnp.float32)]
    return call(collect_kernel, (*weights, *values, sums, scales), outs)[0]


def last_weights(counts, queries, keys, tops, totals):
    rows = queries.shape[0]
    outs = [((HEADS, rows, rows), jnp.bfloat16), ((PAIRS, rows, LANES), jnp.float32)]
    return call(weights_kernel, (counts, queries, keys, tops, totals), outs)


def finish(shares, values, most, counts):
    outs = [((LATENT_CH, most.shape[0]), jnp.float32), ((1, LANES), jnp.float32)]
    return call(finish_kernel, (shares, values, most, counts), outs)


def exchange(shard, pairs):
    return lax.ppermute(shard, BLK, pairs)


def exchanged_sum(copies, axes):
    gathered = lax.all_to_all(copies, axes, 0, 0, tiled=True)
    return jnp.sum(gathered, axis=0, keepdims=True)


def step(queries, keys, values, out_weight, latent, valid, timestep):
    blocks = lax.axis_size(BLK)
    own = lax.axis_index(BLK)
    near_pairs = [((i + 2) % blocks if i % 2 == 0 else (i - 2) % blocks, i) for i in range(blocks)]
    far_pairs = [((i - 2) % blocks if i % 2 == 0 else (i + 2) % blocks, i) for i in range(blocks)]
    chip_pairs = [(i, i ^ 1) for i in range(blocks)]
    is_odd = own % 2
    partner = own + 1 - 2 * is_odd
    near = own + 2 - 4 * is_odd
    far = own - 2 + 4 * is_odd
    over = own - 1 + 2 * is_odd
    index = jnp.stack([own, partner, near, far, over])
    inside = (index >= 0) & (index < blocks)
    counts = jnp.where(inside, valid[jnp.clip(index, 0, blocks - 1)], 0).astype(jnp.int32)
    counts = jnp.broadcast_to(counts[:, None], (len(index), LANES))

    keys_near = exchange(keys, near_pairs)
    keys_far = exchange(keys, far_pairs)
    keys_partner = exchange(keys, chip_pairs)
    projected = project(counts, values, out_weight)
    projected_near = exchange(projected, near_pairs)
    projected_partner = exchange(projected, chip_pairs)
    own_sums, own_tops, own_totals = own_attention(
        counts, queries, (keys, keys_partner), (projected, projected_partner)
    )
    projected, own_sums = lax.optimization_barrier((projected, own_sums))
    projected_far = exchange(projected, far_pairs)
    keys_over = exchange(keys_near, chip_pairs)
    weights_near, weights_over, sums, tops, totals = merge(
        counts, queries, (keys_near, keys_over), (own_sums, own_tops, own_totals)
    )
    projected_near, sums = lax.optimization_barrier((projected_near, sums))
    projected_over = exchange(projected_near, chip_pairs)
    shares, scales = last_weights(counts, queries, keys_far, tops, totals)
    most = collect(
        (weights_near, weights_over), (projected_near, projected_over), sums, scales
    )
    vel, squares = finish(shares, projected_far, most, counts)

    columns = lax.axis_size("blk_1")
    moved = [
        lax.ppermute(squares, "blk_1", [(i, (i + by) % columns) for i in range(columns)])
        for by in range(1, columns)
    ]
    squares = functools.reduce(jnp.add, moved, squares)
    count = jnp.float32(LATENT_CH) * jnp.sum(valid.astype(jnp.float32))
    level = timestep[0].astype(jnp.float32)
    early = 1.0 - level / STEPS
    later = 1.0 - (level + 1.0) / STEPS
    sigma_early = 5.0 * early / (1.0 + 4.0 * early)
    sigma_later = 5.0 * later / (1.0 + 4.0 * later)
    copies = jnp.broadcast_to(squares, (lax.axis_size(Z_CORE), LANES))
    copies, count, change = lax.optimization_barrier((copies, count, sigma_later - sigma_early))
    squares = exchanged_sum(copies, Z_CORE)[0, 0]
    rms = jnp.sqrt(squares / count + 1e-06)
    velocity = vel / rms
    return (velocity, latent + change * velocity)


def solution(mesh):
    split = Mesh(
        mesh.devices.reshape(mesh.shape["groups"], 16, 4, 2), ("groups", "blk_0", "blk_1", "blk_2")
    )
    return jax.shard_map(
        step,
        mesh=split,
        in_specs=(
            P(GROUPS_BLK, None),
            P(GROUPS_BLK, None),
            P(GROUPS_BLK, None),
            P(),
            P(None, GROUPS_BLK),
            P("groups"),
            P("groups"),
        ),
        out_specs=(P(None, GROUPS_BLK), P(None, GROUPS_BLK)),
        check_vma=False,
    )
```
